32 devices in a mesh: context: 2 (over core), tensor: 4 (over y, x), fsdp: 4 (over z).
Axes of the slice: x: 2, y: 2, z: 4, core: 2. Of those that a mesh axis runs over, the one named last changes fastest.
Arguments:
- input_raw: bfloat16 [4, 1024, 5120], P('fsdp', ('context', 'tensor')), may hold values from -6 to 6
- state_proj_raw: bfloat16 [4, 1024, 256], P('fsdp', ('context', 'tensor')), may hold values from -6 to 6
- gate_branch: bfloat16 [4, 1024, 5120], P('fsdp', ('context', 'tensor')), may hold values from -6 to 6
- step_raw: bfloat16 [4, 1024, 80], P('fsdp', ('context', 'tensor')), may hold values from -6 to 6
- convolution_taps: float32 [4, 5376], replicated, may hold values from -3 to 3
- convolution_bias: float32 [5376], replicated, may hold values from -3 to 3
- step_bias: float32 [80], P('tensor'), may hold values from -1.5 to 0.5
- decay_log_rate: float32 [80], P('tensor'), may hold values from -13 to -2, as said below
- skip_weight: float32 [80], P('tensor'), may hold values from 0.5 to 2
- gated_norm_gain: float32 [5120], P('tensor'), may hold values from 0.1 to 1.9
- output_weight: bfloat16 [5120, 2560], P('tensor', 'fsdp'), may hold values from -0.078125 to 0.078125
- adapter_down: bfloat16 [5120, 16], P('tensor'), may hold values from -0.078125 to 0.078125
- adapter_up: bfloat16 [16, 2560], replicated, may hold values from -0.29882812 to 0.29882812
- cotangent: bfloat16 [4, 1024, 2560], P('fsdp', ('context', 'tensor')), may hold values from -6 to 6
Outputs:
- mixed: bfloat16 [4, 1024, 2560], P('fsdp', ('context', 'tensor'))
- grad_a: float32 [5120, 16], P('tensor')
- grad_b: float32 [16, 2560], replicated
The draws below stay inside these ranges and needn't reach their ends.
Inputs may be any that keep to these rules, and one draw needn't show every extreme that they name: `decay_log_rate`: logarithms of positive decay rates.
All inputs are finite; a program needn't handle non-finite values.
Results may differ from the reference program's by a relative error of at most 0.017.
Values may be sent and summed in bfloat16 or wider, within the bound.
No kernel may reach another device: no remote copies, remote signals or barrier semaphores. Data moves between devices by JAX's collectives and lax.ppermute only.
A program may use at most 128 MiB of HBM per device.

```python
import math
import jax
import jax.numpy as jnp
from jax import lax

MODEL_WIDTH = 2560
H = 80
N = 128
ADAPTER_RANK = 16
CONV = 4
MIXER_WIDTH = 5120
SEQS = 4
LEN = 1024


def draw_decay_log_rate(key, part):
    pick_key, slow_key, fast_key = jax.random.split(jax.random.fold_in(key, 11), 3)
    keep_share = 5
    slow_mask = jax.random.randint(pick_key, (H,), 0, 10) < keep_share
    low_log = jnp.log(0.5 / LEN)
    high_log = jnp.log(2.5 / LEN)
    slow_rate = jax.random.uniform(slow_key, (H,), jnp.float32, low_log, high_log)
    fast_rate = jnp.log(jax.random.uniform(fast_key, (H,), jnp.float32, 1.0 / 60.0, 1.0 / 20.0))
    return jnp.where(slow_mask, slow_rate, fast_rate)


def block_levels(rng, dims, cuts, low, largest):
    gain, own = 1.0, jax.random.fold_in(rng, 6)
    for position, parts in cuts:
        heights = jnp.exp(jax.random.uniform(jax.random.fold_in(own, position), (parts,), jnp.float32, low / len(cuts), largest / len(cuts)))
        gain = gain * jnp.repeat(heights, dims[position] // parts).reshape([-1 if axis == position else 1 for axis in range(len(dims))])
    return gain


def centred(stream_key, dims, width, reach, cuts=(), held_as=jnp.bfloat16):
    level = block_levels(stream_key, dims, cuts, -0.22, 0.18) if cuts else 1.0
    result = jax.random.normal(stream_key, dims, jnp.float32) * width * level
    return jnp.minimum(jnp.maximum(result, -reach), reach).astype(held_as)


def setup_inputs(seed: int = 0) -> dict:
    arg_keys = jax.random.split(jax.random.key(seed), 15)
    input_raw = centred(arg_keys[0], (SEQS, LEN, MIXER_WIDTH), 1.0, 6.0, ((0, 4), (1, 8)))
    state_proj_raw = centred(arg_keys[1], (SEQS, LEN, 2 * N), 1.0, 6.0, ((0, 4), (1, 8)))
    gate_branch = centred(arg_keys[2], (SEQS, LEN, MIXER_WIDTH), 1.0, 6.0, ((0, 4), (1, 8)))
    step_raw = centred(arg_keys[3], (SEQS, LEN, H), 1.0, 6.0, ((0, 4), (1, 8)))
    convolution_taps = centred(arg_keys[4], (CONV, MIXER_WIDTH + 2 * N), CONV ** -0.5, 3.0, (), jnp.float32)
    convolution_bias = centred(arg_keys[5], (MIXER_WIDTH + 2 * N,), 0.5, 3.0, (), jnp.float32)
    step_bias = jnp.clip(-1.5 + 2.0 * jax.random.uniform(arg_keys[6], (H,), jnp.float32) ** block_levels(arg_keys[6], (H,), ((0, 4),), -0.2, 0.2), -1.5, 0.5)
    decay_log_rate = draw_decay_log_rate(jax.random.fold_in(arg_keys[14], 71), 0)
    skip_weight = jnp.clip(0.5 + 1.5 * jax.random.uniform(arg_keys[8], (H,), jnp.float32) ** block_levels(arg_keys[8], (H,), ((0, 4),), -0.2, 0.2), 0.5, 2.0)
    gated_norm_gain = jnp.clip(1.0 + 0.18 * jax.random.normal(arg_keys[9], (MIXER_WIDTH,), jnp.float32), 0.1, 1.9)
    output_weight = centred(arg_keys[10], (MIXER_WIDTH, MODEL_WIDTH), MIXER_WIDTH ** -0.5, 0.078125, ((0, 4), (1, 4)))
    adapter_down = centred(arg_keys[11], (MIXER_WIDTH, ADAPTER_RANK), MIXER_WIDTH ** -0.5, 0.078125, ((0, 4),))
    adapter_up = centred(arg_keys[12], (ADAPTER_RANK, MODEL_WIDTH), 0.05, 0.29882812)
    cotangent = centred(arg_keys[13], (SEQS, LEN, MODEL_WIDTH), 1.0, 6.0, ((0, 4), (1, 8)))
    return dict(input_raw=input_raw, state_proj_raw=state_proj_raw, gate_branch=gate_branch, step_raw=step_raw, convolution_taps=convolution_taps, convolution_bias=convolution_bias, step_bias=step_bias, decay_log_rate=decay_log_rate, skip_weight=skip_weight, gated_norm_gain=gated_norm_gain, output_weight=output_weight, adapter_down=adapter_down, adapter_up=adapter_up, cotangent=cotangent)


def ssd_blocks(x_heads, b_rows, c_rows, step_size, log_decay, block_len):
    highest = lax.Precision.HIGHEST
    length = x_heads.shape[0]
    head_count = x_heads.shape[1]
    head_size = x_heads.shape[2]
    state_size = b_rows.shape[1]
    blocks = length // block_len
    causal = jnp.arange(block_len)[:, None] >= jnp.arange(block_len)[None, :]

    def advance(state_now, pieces):
        x_block, b_block, c_block, step_block, decay_block = pieces
        cum_decay = jnp.cumsum(decay_block, axis=0)
        cum_heads = cum_decay.T
        gap_decay = cum_heads[:, :, None] - cum_heads[:, None, :]
        decay_mat = jnp.where(causal[None], jnp.exp(jnp.where(causal[None], gap_decay, 0.0)), 0.0)
        gram_mat = jnp.dot(c_block, b_block.T, precision=highest)
        x_scaled = x_block * step_block[:, :, None]
        y_inner = jnp.einsum('hij,jhp->ihp', decay_mat * gram_mat[None], x_scaled, precision=highest)
        y_state = jnp.exp(cum_decay)[:, :, None] * jnp.einsum('in,hpn->ihp', c_block, state_now, precision=highest)
        tail_decay = jnp.exp(cum_decay[-1][None, :] - cum_decay)
        state_next = jnp.exp(cum_decay[-1])[:, None, None] * state_now + jnp.einsum('jhp,jn->hpn', x_scaled * tail_decay[:, :, None], b_block, precision=highest)
        return (state_next, y_inner + y_state)
    start_state = jnp.zeros((head_count, head_size, state_size), jnp.float32)
    state_end, y_blocks = lax.scan(advance, start_state, (x_heads.reshape(blocks, block_len, head_count, head_size), b_rows.reshape(blocks, block_len, state_size), c_rows.reshape(blocks, block_len, state_size), step_size.reshape(blocks, block_len, head_count), log_decay.reshape(blocks, block_len, head_count)))
    return (y_blocks.reshape(length, head_count, head_size), state_end)

def reference(input_raw, state_proj_raw, gate_branch, step_raw, convolution_taps, convolution_bias, step_bias, decay_log_rate, skip_weight, gated_norm_gain, output_weight, adapter_down, adapter_up, cotangent):
    highest = lax.Precision.HIGHEST
    inner_width = input_raw.shape[2]
    state_size = state_proj_raw.shape[2] // 2
    head_count = decay_log_rate.shape[0]
    head_size = inner_width // head_count
    length = input_raw.shape[1]
    taps = convolution_taps.shape[0]
    block_len = math.gcd(length, 256)
    lowrank_factor = 2.0 / math.sqrt(input_raw.shape[0] * length)
    decay_rate = jnp.exp(decay_log_rate)

    def one_sequence(pieces):
        x_seq, bc_seq, z_seq, dt_seq, cotangent_sequence = pieces
        joined = jnp.concatenate([x_seq, bc_seq], axis=1)
        padded = jnp.concatenate([jnp.zeros((taps - 1, joined.shape[1]), joined.dtype), joined], axis=0)
        pre_act = convolution_bias[None, :] + convolution_taps[0][None, :] * padded[0:length].astype(jnp.float32)
        for tap_index in range(1, taps):
            pre_act = pre_act + convolution_taps[tap_index][None, :] * padded[tap_index:tap_index + length].astype(jnp.float32)
        xbc = jax.nn.silu(pre_act).astype(jnp.bfloat16)
        x_heads = xbc[:, :inner_width].astype(jnp.float32).reshape(length, head_count, head_size)
        b_rows = xbc[:, inner_width:inner_width + state_size].astype(jnp.float32)
        c_rows = xbc[:, inner_width + state_size:].astype(jnp.float32)
        step_size = jax.nn.softplus(dt_seq.astype(jnp.float32) + step_bias[None, :])
        log_decay = -step_size * decay_rate[None, :]
        y_heads, state_end = ssd_blocks(x_heads, b_rows, c_rows, step_size, log_decay, block_len)
        y_heads = y_heads + skip_weight[None, :, None] * x_heads
        gated = y_heads.reshape(length, inner_width) * jax.nn.silu(z_seq.astype(jnp.float32))
        row_norm_scale = lax.rsqrt(lax.optimization_barrier(jnp.mean(gated * gated, axis=1)) + 1e-05)
        gated_output = (gated * gated_norm_gain[None, :]).astype(jnp.bfloat16)
        adapter_branch = jnp.dot(gated_output, adapter_down, preferred_element_type=jnp.float32).astype(jnp.bfloat16)
        frozen_piece = jnp.dot(gated_output, output_weight, preferred_element_type=jnp.float32)
        frozen_piece = frozen_piece + 2.0 * jnp.dot(adapter_branch, adapter_up, preferred_element_type=jnp.float32)
        mixed = (row_norm_scale[:, None] * frozen_piece).astype(jnp.bfloat16)
        weighted = lowrank_factor * row_norm_scale[:, None] * adapter_branch.astype(jnp.float32)
        grad_b_part = jnp.dot(weighted.T, cotangent_sequence.astype(jnp.float32), precision=highest)
        adapter_gradient = lowrank_factor * row_norm_scale[:, None] * jnp.dot(cotangent_sequence, adapter_up.T, preferred_element_type=jnp.float32)
        grad_a_part = jnp.dot(gated_output.astype(jnp.float32).T, adapter_gradient, precision=highest)
        return (mixed, grad_a_part, grad_b_part)
    mixed, grad_a_parts, grad_b_parts = lax.map(one_sequence, (input_raw, state_proj_raw, gate_branch, step_raw, cotangent))
    return (mixed, lax.optimization_barrier(jnp.sum(grad_a_parts, axis=0)), lax.optimization_barrier(jnp.sum(grad_b_parts, axis=0)))
```

```python
import functools
import math

import jax
import jax.numpy as jnp
from jax import lax
from jax.experimental import pallas as pl
from jax.experimental.pallas import tpu as pltpu
from jax.sharding import PartitionSpec as P

epsilon = 1e-05
LANES = 128
f32, bf16 = jnp.float32, jnp.bfloat16
HIGHEST = lax.Precision.HIGHEST


def exchange(value, axis):
    return lax.all_to_all(value, axis, split_axis=0, concat_axis=0, tiled=False)


def spread(value, axis, count):
    return exchange(jnp.broadcast_to(value[None], (count,) + value.shape), axis)


def silu(value):
    return 0.5 * value * (1.0 + jnp.tanh(0.5 * value))


def dot_nt(a, b, precision=None):
    return lax.dot_general(a, b, (((1,), (1,)), ((), ())), precision=precision, preferred_element_type=f32)


def dot_tn(a, b, precision=None):
    return lax.dot_general(a, b, (((0,), (0,)), ((), ())), precision=precision, preferred_element_type=f32)


def dot_nn(a, b, precision=None):
    return jnp.dot(a, b, precision=precision, preferred_element_type=f32)


def paired(table, pair, low_half, shape):
    first = jnp.broadcast_to(table[:, 2 * pair : 2 * pair + 1], shape)
    second = jnp.broadcast_to(table[:, 2 * pair + 1 : 2 * pair + 2], shape)
    return jnp.where(low_half, first, second)


def states_body(width, state, chunk, blocks, raw, rim, taps, bias, step_bias, rate, xconv, bc_out, step_out, cum_out, cumt_out, end_out, total_out, prev):
    joint = width + 2 * state
    prev[...] = rim[...].astype(f32)
    end_out[...] = jnp.zeros_like(end_out)
    total_out[...] = jnp.zeros_like(total_out)
    rows = lax.broadcasted_iota(jnp.int32, (chunk, chunk), 0)
    cols = lax.broadcasted_iota(jnp.int32, (chunk, chunk), 1)
    lower = (rows >= cols).astype(f32)
    low_half = lax.broadcasted_iota(jnp.int32, (chunk, LANES), 1) < LANES // 2
    low_row = lax.broadcasted_iota(jnp.int32, (1, LANES), 1) < LANES // 2
    count = taps.shape[0]

    def convolved(block, start):
        part = pl.ds(start, LANES)
        here = raw[block, :, part].astype(f32)
        cat = jnp.concatenate([prev[:, part], here], axis=0)
        total = bias[0:1, part] + taps[count - 1 : count, part] * here
        for k in range(count - 1):
            shift = 8 - (count - 1) + k
            total = total + taps[k : k + 1, part] * cat[shift : shift + chunk]
        prev[:, part] = here[chunk - 8 :]
        return silu(total).astype(bf16)

    def one(block, carry):
        log_steps = raw[block, :, joint : joint + LANES].astype(f32) + step_bias[...]
        step = jnp.maximum(log_steps, 0.0) + jnp.log1p(jnp.exp(-jnp.abs(log_steps)))
        decay = -step * rate[...]
        cum = dot_nn(lower, decay, HIGHEST)
        cumt = dot_tn(decay, (rows <= cols).astype(f32), HIGHEST)
        step_out[block] = step
        cum_out[block] = cum
        cumt_out[block] = cumt[: cumt_out.shape[1]]
        last = cum[chunk - 1 : chunk]
        tail = step * jnp.exp(last - cum)
        whole = jnp.exp(last)
        total_out[...] = total_out[...] + last
        for start in range(width, joint, LANES):
            bc_out[block, :, start - width : start - width + LANES] = convolved(block, start)
        b_t = bc_out[block, :, 0:state].T
        for pair in range(width // LANES):
            part = pl.ds(pair * LANES, LANES)
            x = convolved(block, pair * LANES)
            xconv[block, :, part] = x
            scaled = (x.astype(f32) * paired(tail, pair, low_half, (chunk, LANES))).astype(bf16)
            end_out[:, part] = paired(whole, pair, low_row, (1, LANES)) * end_out[:, part] + dot_nn(b_t, scaled)
        return carry

    lax.fori_loop(0, blocks, one, 0)


def outputs_body(width, state, chunk, blocks, xconv, bc, step_in, cum_in, cumt_in, start_state, gate, skip, gain, down_t, gated_out, stats, now):
    now[...] = start_state[...]
    rows = lax.broadcasted_iota(jnp.int32, (chunk, chunk), 0)
    cols = lax.broadcasted_iota(jnp.int32, (chunk, chunk), 1)
    causal = rows >= cols
    low_half = lax.broadcasted_iota(jnp.int32, (chunk, LANES), 1) < LANES // 2
    low_row = lax.broadcasted_iota(jnp.int32, (1, LANES), 1) < LANES // 2
    rank = down_t.shape[0]

    def one(block, carry):
        b_rows = bc[block, :, 0:state]
        c_rows = bc[block, :, state : 2 * state]
        b_t = b_rows.T
        gram = dot_nt(c_rows, b_rows)
        step = step_in[block]
        cum = cum_in[block]
        cumt = cumt_in[block]
        last = cum[chunk - 1 : chunk]
        reach = jnp.exp(cum)
        fade = jnp.exp(last - cum)
        whole = jnp.exp(last)
        squares = jnp.zeros((chunk, LANES), f32)
        for pair in range(width // LANES):
            part = pl.ds(pair * LANES, LANES)
            x = xconv[block, :, part].astype(f32)
            scaled = x * paired(step, pair, low_half, (chunk, LANES))
            mats = []
            for head in (2 * pair, 2 * pair + 1):
                gap = cum[:, head : head + 1] - cumt[head : head + 1, :]
                mats.append((jnp.exp(jnp.where(causal, gap, -jnp.inf)) * gram).astype(bf16))
            mat = jnp.concatenate(mats, axis=1)
            stacked = jnp.concatenate([jnp.where(low_half, scaled, 0.0), jnp.where(low_half, 0.0, scaled)], axis=0)
            y = dot_nn(mat, stacked.astype(bf16))
            old = now[:, part]
            y = y + paired(reach, pair, low_half, (chunk, LANES)) * dot_nn(c_rows, old.astype(bf16))
            faded = (scaled * paired(fade, pair, low_half, (chunk, LANES))).astype(bf16)
            now[:, part] = paired(whole, pair, low_row, (1, LANES)) * old + dot_nn(b_t, faded)
            y = y + skip[0:1, part] * x
            gated = y * silu(gate[block, :, part].astype(f32))
            squares = squares + gated * gated
            gated_out[block, :, part] = (gated * gain[0:1, part]).astype(bf16)
        stats[block, 0:rank] = dot_nt(down_t[...], gated_out[block])
        stats[block, rank : rank + 8] = dot_nt(jnp.ones((8, LANES), f32), squares, HIGHEST)
        return carry

    lax.fori_loop(0, blocks, one, 0)


def starting_state(state_end, total_row, heads):
    count = lax.axis_size("context")
    if count == 1:
        return jnp.zeros_like(state_end)
    if count == 2:
        return lax.ppermute(state_end, "context", [(0, 1)])
    mine = lax.axis_index("context")
    ends = lax.all_gather(state_end, "context")
    decays = lax.all_gather(total_row, "context")
    repeated = state_end.shape[1] // heads

    def lap(position, so_far):
        factor = jnp.repeat(jnp.exp(decays[position, :heads]), repeated)
        longer = factor[None, :] * so_far + ends[position]
        return jnp.where(position < mine, longer, so_far)

    return lax.fori_loop(0, count - 1, lap, jnp.zeros_like(state_end))


def shards(
    input_raw,
    state_proj_raw,
    gate_branch,
    step_raw,
    convolution_taps,
    convolution_bias,
    step_bias,
    decay_log_rate,
    skip_weight,
    gated_norm_gain,
    output_weight,
    adapter_down,
    adapter_up,
    cotangent,
):
    chunk = input_raw.shape[1]
    inner_width = input_raw.shape[2]
    state = state_proj_raw.shape[2] // 2
    taps = convolution_taps.shape[0]
    heads = step_bias.shape[0]
    width = gated_norm_gain.shape[0]
    head_size = width // heads
    model = cotangent.shape[2]
    rank = adapter_up.shape[0]
    tensor = lax.axis_size("tensor")
    context = lax.axis_size("context")
    fsdp = lax.axis_size("fsdp")
    mine = lax.axis_index("tensor")
    joint = width + 2 * state

    def by_group(values):
        return values.reshape(values.shape[0], tensor, -1).transpose(1, 0, 2)

    shared = jnp.broadcast_to(state_proj_raw, (tensor, chunk, 2 * state))
    steps = jnp.pad(by_group(step_raw[0]), ((0, 0), (0, 0), (0, LANES - heads)))
    raw = exchange(jnp.concatenate([by_group(input_raw[0]), shared, steps], axis=2), "tensor")
    edge = jnp.concatenate([by_group(input_raw[0, chunk - 8 :]), shared[:, chunk - 8 :]], axis=2)
    edges = jnp.broadcast_to(edge[None], (context,) + edge.shape).reshape((context * tensor,) + edge.shape[1:])
    edges = exchange(edges, ("context", "tensor"))
    place = lax.axis_index("context")
    rim = lax.dynamic_index_in_dim(edges, jnp.maximum(place * tensor - 1, 0), 0, keepdims=False)
    rim = jnp.where(place > 0, rim, jnp.zeros_like(rim))
    late = exchange(jnp.concatenate([by_group(gate_branch[0]), by_group(cotangent[0])], axis=2), "tensor")
    halves = 2 if context % 2 == 0 else 1
    half_rows = width // halves
    parity = place % halves
    own_half = lax.dynamic_slice_in_dim(output_weight, parity * half_rows, half_rows, 0)
    gathered = spread(own_half, "fsdp", fsdp)
    if halves == 2:
        other = lax.ppermute(gathered, "context", [(i, i ^ 1) for i in range(context)])
        gathered = jnp.concatenate([gathered, other], axis=1)
    columns = gathered.transpose(1, 0, 2).reshape(width, model)

    group = lambda values: lax.dynamic_slice_in_dim(values, mine * width, width, values.ndim - 1)
    taps_here = jnp.concatenate([group(convolution_taps), convolution_taps[:, inner_width:]], axis=1)
    bias_here = jnp.concatenate([group(convolution_bias), convolution_bias[inner_width:]])[None]
    row = lambda values: jnp.pad(values, (0, LANES - heads))[None]
    head_rows = -(-heads // 8) * 8
    vmem = pltpu.CompilerParams(vmem_limit_bytes=48 * 2**20)
    sds = jax.ShapeDtypeStruct
    xconv, bc, step, cum, cumt, state_end, total = pl.pallas_call(
        functools.partial(states_body, width, state, chunk, tensor),
        out_shape=(
            sds((tensor, chunk, width), bf16),
            sds((tensor, chunk, 2 * state), bf16),
            sds((tensor, chunk, LANES), f32),
            sds((tensor, chunk, LANES), f32),
            sds((tensor, head_rows, chunk), f32),
            sds((state, width), f32),
            sds((1, LANES), f32),
        ),
        scratch_shapes=[pltpu.VMEM((8, joint), f32)],
        compiler_params=vmem,
        name="span_states",
    )(raw, rim, taps_here, bias_here, row(step_bias), row(jnp.exp(decay_log_rate)))
    start_state = starting_state(state_end, total[0], heads)
    gated_out, stats = pl.pallas_call(
        functools.partial(outputs_body, width, state, chunk, tensor),
        out_shape=(sds((tensor, chunk, width), bf16), sds((tensor, rank + 8, chunk), f32)),
        scratch_shapes=[pltpu.VMEM((state, width), f32)],
        compiler_params=vmem,
        name="span_outputs",
    )(
        xconv, bc, step, cum, cumt, start_state, late[:, :, :width],
        jnp.repeat(skip_weight, head_size)[None], gated_norm_gain[None], adapter_down.T,
    )

    cot_rank = dot_nt(adapter_up, cotangent[0])
    packed = jnp.concatenate([stats.reshape(tensor * (rank + 8), chunk), cot_rank], axis=0)
    packed = spread(packed, "tensor", tensor)
    sums = jnp.sum(packed[:, : tensor * (rank + 8)], axis=0).reshape(tensor, rank + 8, chunk)
    scale = lax.rsqrt(sums[:, rank] / inner_width + epsilon)
    adapter = sums[:, :rank].astype(bf16)
    factor = 2.0 / math.sqrt(chunk * context * tensor * fsdp)
    weighted = (factor * scale[:, None, :] * adapter.astype(f32)).transpose(1, 0, 2).reshape(rank, -1)
    grad_rows = (factor * scale[:, None, :] * packed[:, tensor * (rank + 8) :]).transpose(1, 0, 2).reshape(rank, -1)

    span = tensor * chunk
    flat = gated_out.reshape(span, width)
    if halves == 2:
        ordered = jnp.concatenate(
            [lax.dynamic_slice_in_dim(flat, half * half_rows, half_rows, 1) for half in (parity, 1 - parity)], axis=1
        )
    else:
        ordered = flat
    frozen = dot_nn(ordered, columns).astype(bf16).reshape(tensor, chunk, model)
    pieces = exchange(frozen, "tensor")

    grad_b_part = dot_nn(weighted.astype(bf16), late[:, :, width:].reshape(span, -1))
    grad_a_part = dot_nn(grad_rows.astype(bf16), flat)
    both = spread(jnp.concatenate([grad_a_part, grad_b_part], axis=1), ("context", "fsdp"), context * fsdp)
    both = jnp.sum(both, axis=0)
    grad_a = both[:, :width].T
    grad_b = spread(both[:, width:], "tensor", tensor).transpose(1, 0, 2).reshape(rank, model)

    own_scale = lax.dynamic_index_in_dim(scale, mine, 0, keepdims=False)
    own_adapter = lax.dynamic_index_in_dim(adapter, mine, 0, keepdims=False)
    summed = jnp.sum(pieces.astype(f32), axis=0) + 2.0 * dot_tn(own_adapter, adapter_up)
    mixed = (own_scale[:, None] * summed).astype(bf16)
    return (mixed[None], grad_a, grad_b)


def solution(mesh):
    placed = (
        P("fsdp", ("context", "tensor"), None),
        P("fsdp", ("context", "tensor"), None),
        P("fsdp", ("context", "tensor"), None),
        P("fsdp", ("context", "tensor"), None),
        P(),
        P(),
        P("tensor"),
        P("tensor"),
        P("tensor"),
        P("tensor"),
        P("tensor", "fsdp"),
        P("tensor", None),
        P(),
        P("fsdp", ("context", "tensor"), None),
    )
    return jax.shard_map(
        shards,
        mesh=mesh,
        in_specs=placed,
        out_specs=(P("fsdp", ("context", "tensor"), None), P("tensor", None), P()),
        check_vma=False,
    )
```

```python
import functools
import math

import jax
import jax.numpy as jnp
from jax import lax
from jax.experimental import pallas as pl
from jax.experimental.pallas import tpu as pltpu
from jax.sharding import PartitionSpec as P


epsilon = 1e-05
LANES = 128
f32, bf16 = jnp.float32, jnp.bfloat16
HIGHEST = lax.Precision.HIGHEST


def exchange(value, axis):
    return lax.all_to_all(value, axis, split_axis=0, concat_axis=0, tiled=False)


def spread(value, axis, count):
    return exchange(jnp.broadcast_to(value[None], (count,) + value.shape), axis)


def partner(index, step, count):
    return index ^ step if count & (count - 1) == 0 else (index + step) % count


def sender(index, step, count):
    return index ^ step if count & (count - 1) == 0 else (index - step) % count


def hop(value, axis, step, count):
    return lax.ppermute(value, axis, [(i, partner(i, step, count)) for i in range(count)])


def after(values, earlier):
    return lax.optimization_barrier((values, earlier))[0]


def along(value, axis, step):
    count = lax.axis_size(axis)
    return lax.ppermute(value, axis, [(i, i + step) for i in range(count) if 0 <= i + step < count])


def pack_body(group_sizes, shared_sizes, *refs):
    out = refs[-1]
    parts = refs[: len(group_sizes)]
    shared = refs[len(group_sizes) : -1]
    order = [(parts[0], group_sizes[0], True)]
    order += [(ref, size, False) for ref, size in zip(shared, shared_sizes)]
    order += [(ref, size, True) for ref, size in zip(parts[1:], group_sizes[1:])]
    for peer in range(out.shape[0]):
        start = 0
        for ref, size, split in order:
            piece = ref[:, peer * size : (peer + 1) * size] if split else ref[...]
            out[peer, :, start : start + size] = piece
            start += size
        if start < out.shape[2]:
            out[peer, :, start:] = jnp.zeros((out.shape[1], out.shape[2] - start), out.dtype)


def packed_for(peers, grouped, shared):
    sizes = [part.shape[1] // peers for part in grouped]
    shared_sizes = [part.shape[1] for part in shared]
    total = -(-(sum(sizes) + sum(shared_sizes)) // LANES) * LANES
    return pl.pallas_call(
        functools.partial(pack_body, sizes, shared_sizes),
        out_shape=jax.ShapeDtypeStruct((peers, grouped[0].shape[0], total), grouped[0].dtype),
    )(*grouped, *shared)


def silu(value):
    return 0.5 * value * (1.0 + jnp.tanh(0.5 * value))


def dot_nt(a, b, precision=None):
    return lax.dot_general(a, b, (((1,), (1,)), ((), ())), precision=precision, preferred_element_type=f32)


def dot_tn(a, b, precision=None):
    return lax.dot_general(a, b, (((0,), (0,)), ((), ())), precision=precision, preferred_element_type=f32)


def dot_nn(a, b, precision=None):
    return jnp.dot(a, b, precision=precision, preferred_element_type=f32)


def paired(table, pair, low_half, shape):
    first = jnp.broadcast_to(table[:, 2 * pair : 2 * pair + 1], shape)
    second = jnp.broadcast_to(table[:, 2 * pair + 1 : 2 * pair + 2], shape)
    return jnp.where(low_half, first, second)


def states_body(width, state, chunk, blocks, raw, rim, taps, bias, step_bias, rate, xconv, bc_out, step_out, cum_out, cumt_out, end_out, total_out, prev):
    joint = width + 2 * state
    prev[...] = rim[...].astype(f32)
    end_out[...] = jnp.zeros_like(end_out)
    total_out[...] = jnp.zeros_like(total_out)
    rows = lax.broadcasted_iota(jnp.int32, (chunk, chunk), 0)
    cols = lax.broadcasted_iota(jnp.int32, (chunk, chunk), 1)
    lower = (rows >= cols).astype(f32)
    low_half = lax.broadcasted_iota(jnp.int32, (chunk, LANES), 1) < LANES // 2
    low_row = lax.broadcasted_iota(jnp.int32, (1, LANES), 1) < LANES // 2
    count = taps.shape[0]

    def convolved(block, start):
        part = pl.ds(start, LANES)
        here = raw[block, :, part].astype(f32)
        cat = jnp.concatenate([prev[:, part], here], axis=0)
        total = bias[0:1, part] + taps[count - 1 : count, part] * here
        for k in range(count - 1):
            shift = 8 - (count - 1) + k
            total = total + taps[k : k + 1, part] * cat[shift : shift + chunk]
        prev[:, part] = here[chunk - 8 :]
        return silu(total).astype(bf16)

    def one(block, carry):
        log_steps = raw[block, :, joint : joint + LANES].astype(f32) + step_bias[...]
        step = jnp.maximum(log_steps, 0.0) + jnp.log1p(jnp.exp(-jnp.abs(log_steps)))
        decay = -step * rate[...]
        cum = dot_nn(lower, decay, HIGHEST)
        cumt = dot_tn(decay, (rows <= cols).astype(f32), HIGHEST)
        step_out[block] = step
        cum_out[block] = cum
        cumt_out[block] = cumt[: cumt_out.shape[1]]
        last = cum[chunk - 1 : chunk]
        tail = step * jnp.exp(last - cum)
        whole = jnp.exp(last)
        total_out[...] = total_out[...] + last
        for start in range(width, joint, LANES):
            bc_out[block, :, start - width : start - width + LANES] = convolved(block, start)
        b_t = bc_out[block, :, 0:state].T
        for pair in range(width // LANES):
            part = pl.ds(pair * LANES, LANES)
            x = convolved(block, pair * LANES)
            xconv[block, :, part] = x
            scaled = (x.astype(f32) * paired(tail, pair, low_half, (chunk, LANES))).astype(bf16)
            end_out[:, part] = paired(whole, pair, low_row, (1, LANES)) * end_out[:, part] + dot_nn(b_t, scaled)
        return carry

    lax.fori_loop(0, blocks, one, 0)


def recurrence_body(width, state, chunk, blocks, xconv, bc, step_in, cum_in, cumt_in, start_state, skip, y_out, now):
    now[...] = start_state[...]
    rows = lax.broadcasted_iota(jnp.int32, (chunk, chunk), 0)
    cols = lax.broadcasted_iota(jnp.int32, (chunk, chunk), 1)
    causal = rows >= cols
    low_half = lax.broadcasted_iota(jnp.int32, (chunk, LANES), 1) < LANES // 2
    low_row = lax.broadcasted_iota(jnp.int32, (1, LANES), 1) < LANES // 2

    def one(block, carry):
        b_rows = bc[block, :, 0:state]
        c_rows = bc[block, :, state : 2 * state]
        b_t = b_rows.T
        gram = dot_nt(c_rows, b_rows)
        step = step_in[block]
        cum = cum_in[block]
        cumt = cumt_in[block]
        last = cum[chunk - 1 : chunk]
        reach = jnp.exp(cum)
        fade = jnp.exp(last - cum)
        whole = jnp.exp(last)
        for pair in range(width // LANES):
            part = pl.ds(pair * LANES, LANES)
            x = xconv[block, :, part].astype(f32)
            scaled = x * paired(step, pair, low_half, (chunk, LANES))
            mats = []
            for head in (2 * pair, 2 * pair + 1):
                gap = cum[:, head : head + 1] - cumt[head : head + 1, :]
                mats.append((jnp.exp(jnp.where(causal, gap, -jnp.inf)) * gram).astype(bf16))
            mat = jnp.concatenate(mats, axis=1)
            stacked = jnp.concatenate([jnp.where(low_half, scaled, 0.0), jnp.where(low_half, 0.0, scaled)], axis=0)
            y = dot_nn(mat, stacked.astype(bf16))
            old = now[:, part]
            y = y + paired(reach, pair, low_half, (chunk, LANES)) * dot_nn(c_rows, old.astype(bf16))
            faded = (scaled * paired(fade, pair, low_half, (chunk, LANES))).astype(bf16)
            now[:, part] = paired(whole, pair, low_row, (1, LANES)) * old + dot_nn(b_t, faded)
            y_out[block, :, part] = y + skip[0:1, part] * x
        return carry

    lax.fori_loop(0, blocks, one, 0)


def gating_body(width, chunk, blocks, y_in, gate, gain, down_t, gated_out, stats):
    rank = down_t.shape[0]

    def one(block, carry):
        squares = jnp.zeros((chunk, LANES), f32)
        for start in range(0, width, LANES):
            part = pl.ds(start, LANES)
            gated = y_in[block, :, part] * silu(gate[block, :, part].astype(f32))
            squares = squares + gated * gated
            gated_out[block, :, part] = (gated * gain[0:1, part]).astype(bf16)
        stats[block, 0:rank] = dot_nt(down_t[...], gated_out[block])
        stats[block, rank : rank + 8] = dot_nt(jnp.ones((8, LANES), f32), squares, HIGHEST)
        return carry

    lax.fori_loop(0, blocks, one, 0)


def mixed_body(fsdp, tensor, held, spot, scale, adapter, up, *refs):
    out = refs[-1]
    shard = out.shape[1] // fsdp
    for turn, ks in enumerate(held):
        for position, k in enumerate(ks):
            total = 0.0
            for ref in refs[turn * tensor : (turn + 1) * tensor]:
                total = total + ref[:, position * shard : (position + 1) * shard].astype(f32)
            place = pl.ds(pl.multiple_of(lax.rem(spot[0] + k, fsdp) * shard, LANES), shard)
            total = total + 2.0 * dot_tn(adapter[...], up[:, place])
            out[:, place] = (scale[...] * total).astype(bf16)


def starting_state(state_end, total_row, heads):
    count = lax.axis_size("context")
    if count == 1:
        return jnp.zeros_like(state_end)
    if count == 2:
        return lax.ppermute(state_end, "context", [(0, 1)])
    mine = lax.axis_index("context")
    ends = lax.all_gather(state_end, "context")
    decays = lax.all_gather(total_row, "context")
    repeated = state_end.shape[1] // heads

    def lap(position, so_far):
        factor = jnp.repeat(jnp.exp(decays[position, :heads]), repeated)
        longer = factor[None, :] * so_far + ends[position]
        return jnp.where(position < mine, longer, so_far)

    return lax.fori_loop(0, count - 1, lap, jnp.zeros_like(state_end))


def shards(
    input_raw,
    state_proj_raw,
    gate_branch,
    step_raw,
    convolution_taps,
    convolution_bias,
    step_bias,
    decay_log_rate,
    skip_weight,
    gated_norm_gain,
    output_weight,
    adapter_down,
    adapter_up,
    cotangent,
):
    chunk = input_raw.shape[1]
    inner_width = input_raw.shape[2]
    state = state_proj_raw.shape[2] // 2
    heads = step_bias.shape[0]
    width = gated_norm_gain.shape[0]
    head_size = width // heads
    model = cotangent.shape[2]
    rank = adapter_up.shape[0]
    tensor = lax.axis_size("tensor")
    context = lax.axis_size("context")
    fsdp = lax.axis_size("fsdp")
    mine = lax.axis_index("tensor")
    joint = width + 2 * state

    def pieces_of(product):
        return [lax.dynamic_index_in_dim(product, partner(mine, k, tensor), 0, keepdims=False) for k in range(tensor)]

    def over_groups(pieces):
        return [pieces[0]] + [hop(pieces[k], "tensor", k, tensor) for k in reversed(range(1, tensor))]

    raw = exchange(packed_for(tensor, [input_raw[0], step_raw[0]], [state_proj_raw[0]]), "tensor")
    rim = along(raw[tensor - 1, chunk - 8 :, :joint], "context", 1)
    place = lax.axis_index("context")
    packed_gate = packed_for(tensor, [gate_branch[0]], [])
    gate = exchange(packed_gate, "tensor")
    halves = 2 if context % 2 == 0 else 1
    half_rows = width // halves
    parity = place % halves
    own_half = lax.dynamic_slice_in_dim(output_weight, parity * half_rows, half_rows, 0)
    rising, falling = [own_half], [own_half]
    rising.append(along(own_half, "fsdp", 1))
    falling.append(along(own_half, "fsdp", -1))

    group = lambda values: lax.dynamic_slice_in_dim(values, mine * width, width, values.ndim - 1)
    taps_here = jnp.concatenate([group(convolution_taps), convolution_taps[:, inner_width:]], axis=1)
    bias_here = jnp.concatenate([group(convolution_bias), convolution_bias[inner_width:]])[None]
    row = lambda values: jnp.pad(values, (0, LANES - heads))[None]
    head_rows = -(-heads // 8) * 8
    vmem = pltpu.CompilerParams(vmem_limit_bytes=48 * 2**20)
    sds = jax.ShapeDtypeStruct
    xconv, bc, step, cum, cumt, state_end, total = pl.pallas_call(
        functools.partial(states_body, width, state, chunk, tensor),
        out_shape=(
            sds((tensor, chunk, width), bf16),
            sds((tensor, chunk, 2 * state), bf16),
            sds((tensor, chunk, LANES), f32),
            sds((tensor, chunk, LANES), f32),
            sds((tensor, head_rows, chunk), f32),
            sds((state, width), f32),
            sds((1, LANES), f32),
        ),
        scratch_shapes=[pltpu.VMEM((8, joint), f32)],
        compiler_params=vmem,
        name="span_states",
    )(raw, rim, taps_here, bias_here, row(step_bias), row(jnp.exp(decay_log_rate)))
    start_state = starting_state(state_end, total[0], heads)
    y = pl.pallas_call(
        functools.partial(recurrence_body, width, state, chunk, tensor),
        out_shape=sds((tensor, chunk, width), f32),
        scratch_shapes=[pltpu.VMEM((state, width), f32)],
        compiler_params=vmem,
        name="span_recurrence",
    )(xconv, bc, step, cum, cumt, start_state, jnp.repeat(skip_weight, head_size)[None])
    packed_turn = after(packed_for(tensor, [cotangent[0]], []), y)
    turned = exchange(packed_turn, "tensor")
    waits = {1: raw, 2: y}
    for step_index in range(1, fsdp - 1):
        last_two = (rising[-1], falling[-1])
        if step_index in waits:
            last_two = after(last_two, waits[step_index])
        rising.append(along(last_two[0], "fsdp", 1))
        falling.append(along(last_two[1], "fsdp", -1))
    ranked = sorted(range(fsdp), key=lambda k: (max(k, fsdp - k) if k else 0, k))
    early, rest = ranked[: max(1, fsdp // 2)], ranked[max(1, fsdp // 2) :]

    def assembled(ks, ends):
        held = [own_half if k == 0 else ends[1][k] + ends[0][fsdp - k] for k in ks]
        here = jnp.concatenate(held, axis=1)
        if halves == 1:
            return here
        other = lax.ppermute(here, "context", [(i, i ^ 1) for i in range(context)])
        return jnp.concatenate([here, other], axis=0)

    gated_out, stats = pl.pallas_call(
        functools.partial(gating_body, width, chunk, tensor),
        out_shape=(sds((tensor, chunk, width), bf16), sds((tensor, rank + 8, chunk), f32)),
        compiler_params=vmem,
        name="span_gating",
    )(y, gate, gated_norm_gain[None], adapter_down.T)

    cot_rank = dot_nt(adapter_up, cotangent[0])
    packed = jnp.concatenate([stats.reshape(tensor * (rank + 8), chunk), cot_rank], axis=0)
    arrived = {0: packed}
    for k in range(1, tensor):
        arrived[k] = hop(packed, "tensor", k, tensor)
    span = tensor * chunk
    flat = gated_out.reshape(span, width)
    if halves == 2:
        ordered = jnp.concatenate(
            [lax.dynamic_slice_in_dim(flat, half * half_rows, half_rows, 1) for half in (parity, 1 - parity)], axis=1
        )
    else:
        ordered = flat
    columns_early = assembled(early, after((rising[: fsdp // 2 + 1], falling[: fsdp // 2 + 1]), y))
    product_early = dot_nn(ordered, columns_early).astype(bf16).reshape(tensor, chunk, -1)
    pieces_early = pieces_of(product_early)
    parts = over_groups(pieces_early)
    arrived = after(arrived, pieces_early)
    sums = sum(part[: tensor * (rank + 8)] for part in arrived.values()).reshape(tensor, rank + 8, chunk)
    by_source = jnp.stack([arrived[k][tensor * (rank + 8) :] for k in range(tensor)])
    order = [sender(mine, k, tensor) for k in range(tensor)]
    block_index = jnp.arange(tensor)
    rank_rows = sum(
        jnp.where((block_index == order[k])[:, None, None], by_source[k][None], 0.0) for k in range(tensor)
    )
    scale = lax.rsqrt(sums[:, rank] / inner_width + epsilon)
    adapter = sums[:, :rank].astype(bf16)
    factor = 2.0 / math.sqrt(chunk * context * tensor * fsdp)
    weighted = (factor * scale[:, None, :] * adapter.astype(f32)).transpose(1, 0, 2).reshape(rank, -1)
    grad_rows = (factor * scale[:, None, :] * rank_rows).transpose(1, 0, 2).reshape(rank, -1)

    grad_b_part = dot_nn(weighted.astype(bf16), turned.reshape(span, -1))
    grad_a_part = dot_nn(grad_rows.astype(bf16), flat)
    payload = jnp.concatenate([grad_a_part, grad_b_part], axis=1).astype(bf16)
    both = spread(payload, ("context", "fsdp"), context * fsdp)
    both = jnp.sum(both.astype(f32), axis=0)
    grad_a = both[:, :width].T
    grad_b = spread(both[:, width:], "tensor", tensor).transpose(1, 0, 2).reshape(rank, model)

    if rest:
        columns_rest = assembled(rest, after((rising, falling), (payload, pieces_early)))
        product_rest = dot_nn(ordered, columns_rest).astype(bf16).reshape(tensor, chunk, -1)
        parts = parts + over_groups(pieces_of(product_rest))
    own_scale = lax.dynamic_index_in_dim(scale, mine, 0, keepdims=False)
    own_adapter = lax.dynamic_index_in_dim(adapter, mine, 0, keepdims=False)
    spot = jnp.reshape(lax.axis_index("fsdp"), (1,)).astype(jnp.int32)
    in_vmem = pl.BlockSpec(memory_space=pltpu.VMEM)
    mixed = pl.pallas_call(
        functools.partial(mixed_body, fsdp, tensor, (early, rest)),
        in_specs=[pl.BlockSpec(memory_space=pltpu.SMEM)] + [in_vmem] * (3 + len(parts)),
        out_specs=in_vmem,
        out_shape=sds((chunk, model), bf16),
        compiler_params=vmem,
        name="mixed_rows",
    )(spot, own_scale[:, None], own_adapter, adapter_up, *parts)
    return (mixed[None], grad_a, grad_b)


def solution(mesh):
    placed = (
        P("fsdp", ("context", "tensor"), None),
        P("fsdp", ("context", "tensor"), None),
        P("fsdp", ("context", "tensor"), None),
        P("fsdp", ("context", "tensor"), None),
        P(),
        P(),
        P("tensor"),
        P("tensor"),
        P("tensor"),
        P("tensor"),
        P("tensor", "fsdp"),
        P("tensor", None),
        P(),
        P("fsdp", ("context", "tensor"), None),
    )
    return jax.shard_map(
        shards,
        mesh=mesh,
        in_specs=placed,
        out_specs=(P("fsdp", ("context", "tensor"), None), P("tensor", None), P()),
        check_vma=False,
    )
```

```python
import functools
import math

import jax
import jax.numpy as jnp
from jax import lax
from jax.experimental import pallas as pl
from jax.experimental.pallas import tpu as pltpu
from jax.sharding import PartitionSpec as P


epsilon = 1e-05
LANES = 128
f32, bf16 = jnp.float32, jnp.bfloat16
HIGHEST = lax.Precision.HIGHEST


def exchange(value, axis):
    return lax.all_to_all(value, axis, split_axis=0, concat_axis=0, tiled=False)


def spread(value, axis, count):
    return exchange(jnp.broadcast_to(value[None], (count,) + value.shape), axis)


def partner(index, step, count):
    return index ^ step if count & (count - 1) == 0 else (index + step) % count


def sender(index, step, count):
    return index ^ step if count & (count - 1) == 0 else (index - step) % count


def hop(value, axis, step, count):
    return lax.ppermute(value, axis, [(i, partner(i, step, count)) for i in range(count)])


def after(values, earlier):
    return lax.optimization_barrier((values, earlier))[0]


def along(value, axis, step):
    count = lax.axis_size(axis)
    return lax.ppermute(value, axis, [(i, i + step) for i in range(count) if 0 <= i + step < count])


def pack_body(group_sizes, shared_sizes, *refs):
    out = refs[-1]
    parts = refs[: len(group_sizes)]
    shared = refs[len(group_sizes) : -1]
    order = [(parts[0], group_sizes[0], True)]
    order += [(ref, size, False) for ref, size in zip(shared, shared_sizes)]
    order += [(ref, size, True) for ref, size in zip(parts[1:], group_sizes[1:])]
    for peer in range(out.shape[0]):
        start = 0
        for ref, size, split in order:
            piece = ref[:, peer * size : (peer + 1) * size] if split else ref[...]
            out[peer, :, start : start + size] = piece
            start += size
        if start < out.shape[2]:
            out[peer, :, start:] = jnp.zeros((out.shape[1], out.shape[2] - start), out.dtype)


def packed_for(peers, grouped, shared):
    sizes = [part.shape[1] // peers for part in grouped]
    shared_sizes = [part.shape[1] for part in shared]
    total = -(-(sum(sizes) + sum(shared_sizes)) // LANES) * LANES
    return pl.pallas_call(
        functools.partial(pack_body, sizes, shared_sizes),
        out_shape=jax.ShapeDtypeStruct((peers, grouped[0].shape[0], total), grouped[0].dtype),
    )(*grouped, *shared)


def silu(value):
    return 0.5 * value * (1.0 + jnp.tanh(0.5 * value))


def dot_nt(a, b, precision=None):
    return lax.dot_general(a, b, (((1,), (1,)), ((), ())), precision=precision, preferred_element_type=f32)


def dot_tn(a, b, precision=None):
    return lax.dot_general(a, b, (((0,), (0,)), ((), ())), precision=precision, preferred_element_type=f32)


def dot_nn(a, b, precision=None):
    return jnp.dot(a, b, precision=precision, preferred_element_type=f32)


def paired(table, pair, low_half, shape):
    first = jnp.broadcast_to(table[:, 2 * pair : 2 * pair + 1], shape)
    second = jnp.broadcast_to(table[:, 2 * pair + 1 : 2 * pair + 2], shape)
    return jnp.where(low_half, first, second)


def states_body(width, state, chunk, blocks, raw, rim, taps, bias, step_bias, rate, xconv, bc_out, step_out, cum_out, cumt_out, end_out, total_out, prev):
    joint = width + 2 * state
    prev[...] = rim[...].astype(f32)
    end_out[...] = jnp.zeros_like(end_out)
    total_out[...] = jnp.zeros_like(total_out)
    rows = lax.broadcasted_iota(jnp.int32, (chunk, chunk), 0)
    cols = lax.broadcasted_iota(jnp.int32, (chunk, chunk), 1)
    lower = (rows >= cols).astype(f32)
    low_half = lax.broadcasted_iota(jnp.int32, (chunk, LANES), 1) < LANES // 2
    low_row = lax.broadcasted_iota(jnp.int32, (1, LANES), 1) < LANES // 2
    count = taps.shape[0]

    def convolved(block, start):
        part = pl.ds(start, LANES)
        here = raw[block, :, part].astype(f32)
        cat = jnp.concatenate([prev[:, part], here], axis=0)
        total = bias[0:1, part] + taps[count - 1 : count, part] * here
        for k in range(count - 1):
            shift = 8 - (count - 1) + k
            total = total + taps[k : k + 1, part] * cat[shift : shift + chunk]
        prev[:, part] = here[chunk - 8 :]
        return silu(total).astype(bf16)

    def one(block, carry):
        log_steps = raw[block, :, joint : joint + LANES].astype(f32) + step_bias[...]
        step = jnp.maximum(log_steps, 0.0) + jnp.log1p(jnp.exp(-jnp.abs(log_steps)))
        decay = -step * rate[...]
        cum = dot_nn(lower, decay, HIGHEST)
        cumt = dot_tn(decay, (rows <= cols).astype(f32), HIGHEST)
        step_out[block] = step
        cum_out[block] = cum
        cumt_out[block] = cumt[: cumt_out.shape[1]]
        last = cum[chunk - 1 : chunk]
        tail = step * jnp.exp(last - cum)
        whole = jnp.exp(last)
        total_out[...] = total_out[...] + last
        for start in range(width, joint, LANES):
            bc_out[block, :, start - width : start - width + LANES] = convolved(block, start)
        b_t = bc_out[block, :, 0:state].T
        for pair in range(width // LANES):
            part = pl.ds(pair * LANES, LANES)
            x = convolved(block, pair * LANES)
            xconv[block, :, part] = x
            scaled = (x.astype(f32) * paired(tail, pair, low_half, (chunk, LANES))).astype(bf16)
            end_out[:, part] = paired(whole, pair, low_row, (1, LANES)) * end_out[:, part] + dot_nn(b_t, scaled)
        return carry

    lax.fori_loop(0, blocks, one, 0)


def recurrence_body(width, state, chunk, blocks, xconv, bc, step_in, cum_in, cumt_in, start_state, skip, y_out, now):
    now[...] = start_state[...]
    rows = lax.broadcasted_iota(jnp.int32, (chunk, chunk), 0)
    cols = lax.broadcasted_iota(jnp.int32, (chunk, chunk), 1)
    causal = rows >= cols
    low_half = lax.broadcasted_iota(jnp.int32, (chunk, LANES), 1) < LANES // 2
    low_row = lax.broadcasted_iota(jnp.int32, (1, LANES), 1) < LANES // 2

    def one(block, carry):
        b_rows = bc[block, :, 0:state]
        c_rows = bc[block, :, state : 2 * state]
        b_t = b_rows.T
        gram = dot_nt(c_rows, b_rows)
        step = step_in[block]
        cum = cum_in[block]
        cumt = cumt_in[block]
        last = cum[chunk - 1 : chunk]
        reach = jnp.exp(cum)
        fade = jnp.exp(last - cum)
        whole = jnp.exp(last)
        for pair in range(width // LANES):
            part = pl.ds(pair * LANES, LANES)
            x = xconv[block, :, part].astype(f32)
            scaled = x * paired(step, pair, low_half, (chunk, LANES))
            mats = []
            for head in (2 * pair, 2 * pair + 1):
                gap = cum[:, head : head + 1] - cumt[head : head + 1, :]
                mats.append((jnp.exp(jnp.where(causal, gap, -jnp.inf)) * gram).astype(bf16))
            mat = jnp.concatenate(mats, axis=1)
            stacked = jnp.concatenate([jnp.where(low_half, scaled, 0.0), jnp.where(low_half, 0.0, scaled)], axis=0)
            y = dot_nn(mat, stacked.astype(bf16))
            old = now[:, part]
            y = y + paired(reach, pair, low_half, (chunk, LANES)) * dot_nn(c_rows, old.astype(bf16))
            faded = (scaled * paired(fade, pair, low_half, (chunk, LANES))).astype(bf16)
            now[:, part] = paired(whole, pair, low_row, (1, LANES)) * old + dot_nn(b_t, faded)
            y_out[block, :, part] = y + skip[0:1, part] * x
        return carry

    lax.fori_loop(0, blocks, one, 0)


def gating_body(width, chunk, blocks, y_in, gate, gain, down_t, gated_out, stats):
    rank = down_t.shape[0]

    def one(block, carry):
        squares = jnp.zeros((chunk, LANES), f32)
        for start in range(0, width, LANES):
            part = pl.ds(start, LANES)
            gated = y_in[block, :, part] * silu(gate[block, :, part].astype(f32))
            squares = squares + gated * gated
            gated_out[block, :, part] = (gated * gain[0:1, part]).astype(bf16)
        stats[block, 0:rank] = dot_nt(down_t[...], gated_out[block])
        stats[block, rank : rank + 8] = dot_nt(jnp.ones((8, LANES), f32), squares, HIGHEST)
        return carry

    lax.fori_loop(0, blocks, one, 0)


def mixed_body(fsdp, tensor, held, spot, scale, adapter, up, *refs):
    out = refs[-1]
    shard = out.shape[1] // fsdp
    for turn, ks in enumerate(held):
        for position, k in enumerate(ks):
            total = 0.0
            for ref in refs[turn * tensor : (turn + 1) * tensor]:
                total = total + ref[:, position * shard : (position + 1) * shard].astype(f32)
            place = pl.ds(pl.multiple_of(lax.rem(spot[0] + k, fsdp) * shard, LANES), shard)
            total = total + 2.0 * dot_tn(adapter[...], up[:, place])
            out[:, place] = (scale[...] * total).astype(bf16)


def starting_state(state_end, total_row, heads):
    count = lax.axis_size("context")
    if count == 1:
        return jnp.zeros_like(state_end)
    if count == 2:
        return lax.ppermute(state_end, "context", [(0, 1)])
    mine = lax.axis_index("context")
    ends = lax.all_gather(state_end, "context")
    decays = lax.all_gather(total_row, "context")
    repeated = state_end.shape[1] // heads

    def lap(position, so_far):
        factor = jnp.repeat(jnp.exp(decays[position, :heads]), repeated)
        longer = factor[None, :] * so_far + ends[position]
        return jnp.where(position < mine, longer, so_far)

    return lax.fori_loop(0, count - 1, lap, jnp.zeros_like(state_end))


def shards(
    input_raw,
    state_proj_raw,
    gate_branch,
    step_raw,
    convolution_taps,
    convolution_bias,
    step_bias,
    decay_log_rate,
    skip_weight,
    gated_norm_gain,
    output_weight,
    adapter_down,
    adapter_up,
    cotangent,
):
    chunk = input_raw.shape[1]
    inner_width = input_raw.shape[2]
    state = state_proj_raw.shape[2] // 2
    heads = step_bias.shape[0]
    width = gated_norm_gain.shape[0]
    head_size = width // heads
    model = cotangent.shape[2]
    rank = adapter_up.shape[0]
    tensor = lax.axis_size("tensor")
    context = lax.axis_size("context")
    fsdp = lax.axis_size("fsdp")
    mine = lax.axis_index("tensor")
    joint = width + 2 * state

    def pieces_of(product):
        return [lax.dynamic_index_in_dim(product, partner(mine, k, tensor), 0, keepdims=False) for k in range(tensor)]

    def over_groups(pieces):
        return [pieces[0]] + [hop(pieces[k], "tensor", k, tensor) for k in reversed(range(1, tensor))]

    packed_raw = packed_for(tensor, [input_raw[0], step_raw[0]], [state_proj_raw[0]])
    raw = exchange(packed_raw, "tensor")
    rim = along(raw[tensor - 1, chunk - 8 :, :joint], "context", 1)
    place = lax.axis_index("context")
    packed_gate = packed_for(tensor, [gate_branch[0]], [])
    gate = exchange(packed_gate, "tensor")
    halves = 2 if context % 2 == 0 else 1
    half_rows = width // halves
    parity = place % halves
    own_half = lax.dynamic_slice_in_dim(output_weight, parity * half_rows, half_rows, 0)
    rising, falling = [own_half], [own_half]
    rising.append(along(own_half, "fsdp", 1))
    falling.append(along(own_half, "fsdp", -1))

    group = lambda values: lax.dynamic_slice_in_dim(values, mine * width, width, values.ndim - 1)
    taps_here = jnp.concatenate([group(convolution_taps), convolution_taps[:, inner_width:]], axis=1)
    bias_here = jnp.concatenate([group(convolution_bias), convolution_bias[inner_width:]])[None]
    row = lambda values: jnp.pad(values, (0, LANES - heads))[None]
    head_rows = -(-heads // 8) * 8
    vmem = pltpu.CompilerParams(vmem_limit_bytes=48 * 2**20)
    sds = jax.ShapeDtypeStruct
    xconv, bc, step, cum, cumt, state_end, total = pl.pallas_call(
        functools.partial(states_body, width, state, chunk, tensor),
        out_shape=(
            sds((tensor, chunk, width), bf16),
            sds((tensor, chunk, 2 * state), bf16),
            sds((tensor, chunk, LANES), f32),
            sds((tensor, chunk, LANES), f32),
            sds((tensor, head_rows, chunk), f32),
            sds((state, width), f32),
            sds((1, LANES), f32),
        ),
        scratch_shapes=[pltpu.VMEM((8, joint), f32)],
        compiler_params=vmem,
        name="span_states",
    )(raw, rim, taps_here, bias_here, row(step_bias), row(jnp.exp(decay_log_rate)))
    start_state = starting_state(state_end, total[0], heads)
    y = pl.pallas_call(
        functools.partial(recurrence_body, width, state, chunk, tensor),
        out_shape=sds((tensor, chunk, width), f32),
        scratch_shapes=[pltpu.VMEM((state, width), f32)],
        compiler_params=vmem,
        name="span_recurrence",
    )(xconv, bc, step, cum, cumt, start_state, jnp.repeat(skip_weight, head_size)[None])
    packed_turn = packed_for(tensor, [cotangent[0]], [])
    packed_turn = after(packed_turn, y)
    turned = exchange(packed_turn, "tensor")
    waits = {1: raw, 2: y}
    for step_index in range(1, fsdp - 1):
        last_two = (rising[-1], falling[-1])
        if step_index in waits:
            last_two = after(last_two, waits[step_index])
        rising.append(along(last_two[0], "fsdp", 1))
        falling.append(along(last_two[1], "fsdp", -1))
    ranked = sorted(range(fsdp), key=lambda k: (max(k, fsdp - k) if k else 0, k))
    early, rest = ranked[: max(1, fsdp // 2)], ranked[max(1, fsdp // 2) :]

    def assembled(ks, ends):
        held = [own_half if k == 0 else ends[1][k] + ends[0][fsdp - k] for k in ks]
        here = jnp.concatenate(held, axis=1)
        if halves == 1:
            return here
        other = lax.ppermute(here, "context", [(i, i ^ 1) for i in range(context)])
        return jnp.concatenate([here, other], axis=0)

    gated_out, stats = pl.pallas_call(
        functools.partial(gating_body, width, chunk, tensor),
        out_shape=(sds((tensor, chunk, width), bf16), sds((tensor, rank + 8, chunk), f32)),
        compiler_params=vmem,
        name="span_gating",
    )(y, gate, gated_norm_gain[None], adapter_down.T)

    cot_rank = dot_nt(adapter_up, cotangent[0])
    packed = jnp.concatenate([stats.reshape(tensor * (rank + 8), chunk), cot_rank], axis=0)
    arrived = {0: packed}
    for k in range(1, tensor):
        arrived[k] = hop(packed, "tensor", k, tensor)
    span = tensor * chunk
    flat = gated_out.reshape(span, width)
    if halves == 2:
        ordered = jnp.concatenate(
            [lax.dynamic_slice_in_dim(flat, half * half_rows, half_rows, 1) for half in (parity, 1 - parity)], axis=1
        )
    else:
        ordered = flat
    columns_early = assembled(early, after((rising[: fsdp // 2 + 1], falling[: fsdp // 2 + 1]), y))
    product_early = dot_nn(ordered, columns_early).astype(bf16).reshape(tensor, chunk, -1)
    pieces_early = pieces_of(product_early)
    parts = over_groups(pieces_early)
    arrived = after(arrived, pieces_early)
    sums = sum(part[: tensor * (rank + 8)] for part in arrived.values()).reshape(tensor, rank + 8, chunk)
    by_source = jnp.stack([arrived[k][tensor * (rank + 8) :] for k in range(tensor)])
    order = [sender(mine, k, tensor) for k in range(tensor)]
    block_index = jnp.arange(tensor)
    rank_rows = sum(
        jnp.where((block_index == order[k])[:, None, None], by_source[k][None], 0.0) for k in range(tensor)
    )
    scale = lax.rsqrt(sums[:, rank] / inner_width + epsilon)
    adapter = sums[:, :rank].astype(bf16)
    factor = 2.0 / math.sqrt(chunk * context * tensor * fsdp)
    weighted = (factor * scale[:, None, :] * adapter.astype(f32)).transpose(1, 0, 2).reshape(rank, -1)
    grad_rows = (factor * scale[:, None, :] * rank_rows).transpose(1, 0, 2).reshape(rank, -1)

    grad_b_part = dot_nn(weighted.astype(bf16), turned.reshape(span, -1))
    grad_a_part = dot_nn(grad_rows.astype(bf16), flat)
    payload = jnp.concatenate([grad_a_part, grad_b_part], axis=1).astype(bf16)
    both = spread(payload, ("context", "fsdp"), context * fsdp)
    both = jnp.sum(both.astype(f32), axis=0)
    grad_a = both[:, :width].T
    grad_b = spread(both[:, width:], "tensor", tensor).transpose(1, 0, 2).reshape(rank, model)

    if rest:
        columns_rest = assembled(rest, after((rising, falling), (payload, pieces_early)))
        product_rest = dot_nn(ordered, columns_rest).astype(bf16).reshape(tensor, chunk, -1)
        pieces_rest = pieces_of(product_rest)
        parts = parts + over_groups(pieces_rest)
    own_scale = lax.dynamic_index_in_dim(scale, mine, 0, keepdims=False)
    own_adapter = lax.dynamic_index_in_dim(adapter, mine, 0, keepdims=False)
    spot = jnp.reshape(lax.axis_index("fsdp"), (1,)).astype(jnp.int32)
    in_vmem = pl.BlockSpec(memory_space=pltpu.VMEM)
    mixed = pl.pallas_call(
        functools.partial(mixed_body, fsdp, tensor, (early, rest)),
        in_specs=[pl.BlockSpec(memory_space=pltpu.SMEM)] + [in_vmem] * (3 + len(parts)),
        out_specs=in_vmem,
        out_shape=sds((chunk, model), bf16),
        compiler_params=vmem,
        name="mixed_rows",
    )(spot, own_scale[:, None], own_adapter, adapter_up, *parts)
    return (mixed[None], grad_a, grad_b)


def solution(mesh):
    placed = (
        P("fsdp", ("context", "tensor"), None),
        P("fsdp", ("context", "tensor"), None),
        P("fsdp", ("context", "tensor"), None),
        P("fsdp", ("context", "tensor"), None),
        P(),
        P(),
        P("tensor"),
        P("tensor"),
        P("tensor"),
        P("tensor"),
        P("tensor", "fsdp"),
        P("tensor", None),
        P(),
        P("fsdp", ("context", "tensor"), None),
    )
    return jax.shard_map(
        shards,
        mesh=mesh,
        in_specs=placed,
        out_specs=(P("fsdp", ("context", "tensor"), None), P("tensor", None), P()),
        check_vma=False,
    )
```
